32 devices in a mesh: batch: 8 (over y, x, core), shard: 4 (over z).
Axes of the slice: x: 2, y: 2, z: 4, core: 2. Of those that a mesh axis runs over, the one named last changes fastest.
Arguments:
- particles: float32 [8192, 1024], P(('batch', 'shard')), may hold values from -48 to 48
- batch_of: int32 [2, 8192], P(None, ('batch', 'shard')), may hold values from 0 to 7, as said below
- mixture_means: float32 [16, 1024], replicated, may hold values from -3 to 3
- log_weights: float32 [16], replicated, may hold values from -2 to 2
Outputs:
- moved: float32 [8192, 1024], P(('batch', 'shard'))
The draws below stay inside these ranges and needn't reach their ends.
Inputs may be any that keep to these rules, and one draw needn't show every extreme that they name: `batch_of`: in each iteration, the 256 particles of one device hold every batch number equally often, 256 / 8 times each.
All inputs are finite; a program needn't handle non-finite values.
Results may differ from the reference program's by a relative error of at most 0.00011.
Values sent between devices are 32-bit elements; how exact they have to be, the bound alone decides.
A program may use at most 64 MiB of HBM per device.

```python
import jax
import jax.numpy as jnp
from jax import lax

D = 1024
COMPONENTS = 16
ITERS = 2
P_DEV = 256
BATCHES = 8
BATCH_ROWS = 1024
PARTICLES = 8192


def draw_particles(key, part):
    first, second = jax.random.split(key, 2)
    ranks = jax.random.permutation(second, D).astype(jnp.float32) + 1.0
    harmonic = jnp.sum(1.0 / (jnp.arange(D, dtype=jnp.float32) + 1.0))
    column_scale = jnp.sqrt(D / (harmonic * ranks))
    points = jax.random.normal(first, (PARTICLES, D), jnp.float32) * column_scale[None, :]
    return jnp.clip(points, -48.0, 48.0)


def draw_batch_of(key, part):
    devices = PARTICLES // P_DEV
    ranks = jax.random.randint(key, (ITERS, devices, P_DEV), 0, 2 ** 20) * P_DEV + jnp.arange(P_DEV, dtype=jnp.int32)
    ordering = jnp.argsort(ranks, axis=2, stable=True)
    return (ordering % BATCHES).reshape(ITERS, PARTICLES).astype(jnp.int32)


def gaussian(key, extent, width, most, kind=jnp.bfloat16):
    return jnp.clip(width * jax.random.normal(key, extent, jnp.float32), -most, most).astype(kind)


def setup_inputs(seed: int = 0) -> dict:
    streams_of = jax.random.split(jax.random.key(seed), 5)
    return {
        "particles": draw_particles(jax.random.fold_in(streams_of[4], 71), 0),
        "batch_of": draw_batch_of(jax.random.fold_in(streams_of[4], 71), 0),
        "mixture_means": gaussian(streams_of[2], (COMPONENTS, D), 0.5, 3.0, jnp.float32),
        "log_weights": jnp.clip(jax.random.uniform(streams_of[3], (COMPONENTS,), jnp.float32, -2.0, 2.0), -2.0, 2.0),
    }


variance = 4.0
step_size = 32.0


def mixture_score(points, mixture_means, log_weights):
    squares = jnp.sum(points * points, axis=1, keepdims=True)
    crossed = jnp.dot(points, mixture_means.T, precision=lax.Precision.HIGHEST, preferred_element_type=jnp.float32)
    centre_sq = jnp.sum(mixture_means * mixture_means, axis=1)
    logits = log_weights[None, :] - (squares - 2.0 * crossed + centre_sq[None, :]) / (2.0 * variance)
    weights_mix = jax.nn.softmax(logits, axis=1)
    pulled = jnp.dot(weights_mix, mixture_means, precision=lax.Precision.HIGHEST, preferred_element_type=jnp.float32)
    return (pulled - points) / variance


def group_drift(group, mixture_means, log_weights):
    scores = mixture_score(group, mixture_means, log_weights)
    squares = jnp.sum(group * group, axis=1)
    crossed = jnp.dot(group, group.T, precision=lax.Precision.HIGHEST, preferred_element_type=jnp.float32)
    kernel = jnp.exp(-(squares[:, None] + squares[None, :] - 2.0 * crossed) * (2.0 / D))
    acc_score = jnp.dot(kernel, scores, precision=lax.Precision.HIGHEST, preferred_element_type=jnp.float32)
    acc_point = jnp.dot(kernel, group, precision=lax.Precision.HIGHEST, preferred_element_type=jnp.float32)
    kernel_sum = jnp.sum(kernel, axis=1)
    return (acc_score + (4.0 / D) * (group * kernel_sum[:, None] - acc_point)) / BATCH_ROWS


def reference(particles, batch_of, mixture_means, log_weights):
    current = particles
    for iteration in range(ITERS):
        ordering = jnp.argsort(batch_of[iteration], stable=True).astype(jnp.int32)
        grouped = current[ordering].reshape(BATCHES, BATCH_ROWS, D)
        moved = lax.map(lambda group: group + step_size * group_drift(group, mixture_means, log_weights), grouped)
        current = jnp.zeros_like(current).at[ordering].set(moved.reshape(PARTICLES, D))
    return current
```

```python
import functools

import jax
import jax.numpy as jnp
from jax import lax
from jax.experimental import pallas as pl
from jax.experimental.pallas import tpu as pltpu
from jax.sharding import PartitionSpec as P

variance = 4.0
step_size = 32.0
MESH = pl.DeviceIdType.MESH


def split(a):
    high = a.astype(jnp.bfloat16)
    return high, (a - high.astype(jnp.float32)).astype(jnp.bfloat16)


def dot3(a, b, contract):
    dims = (contract, ((), ()))
    one = functools.partial(lax.dot_general, dimension_numbers=dims, preferred_element_type=jnp.float32)
    return one(a[0], b[0]) + (one(a[0], b[1]) + one(a[1], b[0]))


def step_kernel(
    groups,
    shards,
    rows_ref,
    means_ref,
    logw_ref,
    out_ref,
    pool,
    lhs_high,
    lhs_low,
    own_sq,
    acc,
    acc_w,
    acc_k,
    moved,
    own_sem,
    a_send,
    a_recv,
    x_send,
    x_recv,
    c_send,
    c_recv,
    r_send,
    r_recv,
):
    count, width = rows_ref.shape
    chunk = count // groups
    members = shards
    pairs = members // 2
    components = means_ref.shape[0]
    b = lax.axis_index("batch")
    s = lax.axis_index("shard")
    q, t = b // members, b % members
    x, c = t // 2, t % 2
    g = q * shards + s

    def piece(index):
        return pl.ds(pl.multiple_of(index * chunk, chunk), chunk)

    def place(group):
        return (group // shards) * members + t, group % shards

    def mate(j, other):
        return q * members + lax.rem(x + j, pairs) * 2 + (1 - c if other else c), s

    barrier = pltpu.get_barrier_semaphore()
    targets = [place(lax.rem(g + k, groups)) for k in range(1, groups)]
    targets += [mate(j, False) for j in range(1, pairs)] + [mate(0, True)]
    for target in targets:
        pl.semaphore_signal(barrier, inc=1, device_id=target, device_id_type=MESH)
    pl.semaphore_wait(barrier, len(targets))

    own = pltpu.make_async_copy(rows_ref.at[piece(g)], pool.at[t, piece(g)], own_sem.at[0])
    own.start()
    sends = [own]
    for k in range(1, groups):
        to = lax.rem(g + k, groups)
        sends.append(
            pltpu.make_async_remote_copy(
                src_ref=rows_ref.at[piece(to)],
                dst_ref=pool.at[t, piece(g)],
                send_sem=a_send.at[k],
                recv_sem=a_recv.at[k],
                device_id=place(to),
                device_id_type=MESH,
            )
        )
        sends[-1].start()

    def pass_on(j, k, other):
        source = lax.rem(g + groups - k, groups)
        block = lax.rem(x + pairs - (j if other else 0), pairs) * 2 + c
        sem = (c_send, c_recv) if other else (x_send, x_recv)
        copy = pltpu.make_async_remote_copy(
            src_ref=pool.at[block, piece(source)],
            dst_ref=pool.at[block, piece(source)],
            send_sem=sem[0].at[j, k],
            recv_sem=sem[1].at[j, k],
            device_id=mate(0, True) if other else mate(j, False),
            device_id_type=MESH,
        )
        copy.start()
        return copy

    across, inside = {}, {}
    for k in range(groups):
        if k == 0:
            own.wait()
        else:
            sends[k].wait_recv()
        for j in range(1, pairs):
            across[j, k] = pass_on(j, k, False)
        inside[0, k] = pass_on(0, k, True)
        if k >= 2:
            for j in range(1, pairs):
                across[j, k - 2].wait_recv()
                inside[j, k - 2] = pass_on(j, k - 2, True)

    means = means_ref[...]
    mean_parts = split(means)
    mean_sq = jnp.sum(means * means, axis=1, keepdims=True)
    own_rows = pool[t]
    own_parts = split(own_rows)
    lhs_high[0:count, :] = own_parts[0]
    lhs_low[0:count, :] = own_parts[1]
    lhs_high[count:, :] = mean_parts[0]
    lhs_low[count:, :] = mean_parts[1]
    own_sq[...] = jnp.sum(own_rows * own_rows, axis=1, keepdims=True)

    def process(block, first):
        points = pool[block]
        parts = split(points)
        sq = jnp.sum(points * points, axis=1, keepdims=True)
        sq_row = jnp.transpose(jnp.broadcast_to(sq, (count, 128)))[0:1, :]
        crossed = dot3((lhs_high[...], lhs_low[...]), parts, ((1,), (1,)))
        kernel = jnp.exp(-(own_sq[...] + sq_row - 2.0 * crossed[:count]) * (2.0 / width))
        logits = logw_ref[...] - (sq_row - 2.0 * crossed[count:] + mean_sq) / (2.0 * variance)
        weights = jnp.exp(logits - jnp.max(logits, axis=0, keepdims=True))
        weights = weights / jnp.sum(weights, axis=0, keepdims=True)
        kernel_parts = split(kernel)
        point = dot3(kernel_parts, parts, ((1,), (0,)))
        mixed = dot3(kernel_parts, split(weights), ((1,), (1,)))
        total = jnp.sum(kernel, axis=1, keepdims=True)
        if first:
            acc[...] = point
            acc_w[...] = mixed
            acc_k[...] = total
        else:
            acc[...] += point
            acc_w[...] += mixed
            acc_k[...] += total

    process(t, True)

    for k in range(max(groups - 2, 0), groups):
        for j in range(1, pairs):
            across[j, k].wait_recv()
            inside[j, k] = pass_on(j, k, True)
    for j in range(pairs):
        for k in range(groups):
            inside[j, k].wait_recv()

    def rest(i, carry):
        j, h = i // 2, i % 2
        process(lax.rem(x + pairs - j, pairs) * 2 + lax.rem(c + h, 2), False)
        return carry

    lax.fori_loop(1, members, rest, 0)

    size = count * members
    scale = 4.0 / width
    pulled = dot3(split(acc_w[...]), mean_parts, ((1,), (0,)))
    drift = (pulled - acc[...]) / variance + scale * (pool[t] * acc_k[...] - acc[...])
    moved[...] = pool[t] + (step_size / size) * drift

    home = pltpu.make_async_copy(moved.at[piece(g)], out_ref.at[piece(g)], own_sem.at[1])
    back = [home]
    for k in range(1, groups):
        to = lax.rem(g + k, groups)
        back.append(
            pltpu.make_async_remote_copy(
                src_ref=moved.at[piece(to)],
                dst_ref=out_ref.at[piece(g)],
                send_sem=r_send.at[k],
                recv_sem=r_recv.at[k],
                device_id=place(to),
                device_id_type=MESH,
            )
        )
        back[-1].start()
    home.start()
    for copy in sends[1:]:
        copy.wait_send()
    for copy in across.values():
        copy.wait_send()
    for copy in inside.values():
        copy.wait_send()
    home.wait()
    for copy in back[1:]:
        copy.wait()


def step(rows, means, logw, groups, shards):
    count, width = rows.shape
    components = means.shape[0]
    pairs = shards // 2
    dma = pltpu.SemaphoreType.DMA
    return pl.pallas_call(
        functools.partial(step_kernel, groups, shards),
        out_shape=jax.ShapeDtypeStruct((count, width), jnp.float32),
        in_specs=[pl.BlockSpec(memory_space=pltpu.VMEM)] * 3,
        out_specs=pl.BlockSpec(memory_space=pltpu.VMEM),
        scratch_shapes=[
            pltpu.VMEM((shards, count, width), jnp.float32),
            pltpu.VMEM((count + components, width), jnp.bfloat16),
            pltpu.VMEM((count + components, width), jnp.bfloat16),
            pltpu.VMEM((count, 1), jnp.float32),
            pltpu.VMEM((count, width), jnp.float32),
            pltpu.VMEM((count, components), jnp.float32),
            pltpu.VMEM((count, 1), jnp.float32),
            pltpu.VMEM((count, width), jnp.float32),
            dma((2,)),
            dma((groups,)),
            dma((groups,)),
            dma((pairs, groups)),
            dma((pairs, groups)),
            dma((pairs, groups)),
            dma((pairs, groups)),
            dma((groups,)),
            dma((groups,)),
        ],
        compiler_params=pltpu.CompilerParams(
            collective_id=0, has_side_effects=True, vmem_limit_bytes=48 * 1024 * 1024
        ),
    )(rows, means, logw)


def permutation(batch, groups):
    count = batch.shape[0]
    chunk = count // groups
    index = jnp.arange(count, dtype=jnp.int32)
    same = (batch[:, None] == batch[None, :]) & (index[:, None] < index[None, :])
    spot = batch * chunk + jnp.sum(same.astype(jnp.int32), axis=0)
    return (index[:, None] == spot[None, :]).astype(jnp.float32)


def apply(matrix, rows, transposed=False):
    dims = (((0,), (0,)) if transposed else ((1,), (0,)), ((), ()))
    return lax.dot_general(
        matrix, rows, dims, precision=lax.Precision.HIGHEST, preferred_element_type=jnp.float32
    )


def body(particles, batch_of, mixture_means, log_weights):
    groups = lax.axis_size("batch")
    shards = lax.axis_size("shard")
    logw = log_weights[:, None]
    current = particles
    previous = None
    for iteration in range(batch_of.shape[0]):
        order = permutation(batch_of[iteration], groups)
        if previous is None:
            current = apply(order, current)
        else:
            both = lax.dot_general(
                order.astype(jnp.bfloat16),
                previous.astype(jnp.bfloat16),
                (((1,), (1,)), ((), ())),
                preferred_element_type=jnp.float32,
            )
            current = apply(both, current)
        current = step(current, mixture_means, logw, groups, shards)
        previous = order
    return apply(previous, current, transposed=True)


def solution(mesh):
    placed = (P(("batch", "shard"), None), P(None, ("batch", "shard")), P(), P())
    return jax.shard_map(
        body, mesh=mesh, in_specs=placed, out_specs=P(("batch", "shard"), None), check_vma=False
    )
```

```python
import functools

import jax
import jax.numpy as jnp
from jax import lax
from jax.experimental import pallas as pl
from jax.experimental.pallas import tpu as pltpu
from jax.sharding import PartitionSpec as P

variance = 4.0
step_size = 32.0
MESH = pl.DeviceIdType.MESH


def split(a):
    high = a.astype(jnp.bfloat16)
    return high, (a - high.astype(jnp.float32)).astype(jnp.bfloat16)


def dot3(a, b, contract):
    dims = (contract, ((), ()))
    one = functools.partial(lax.dot_general, dimension_numbers=dims, preferred_element_type=jnp.float32)
    return one(a[0], b[0]) + (one(a[0], b[1]) + one(a[1], b[0]))


def step_kernel(
    groups,
    shards,
    rows_ref,
    means_ref,
    logw_ref,
    out_ref,
    pool,
    mine,
    lhs_high,
    lhs_low,
    own_sq,
    acc,
    acc_w,
    acc_k,
    late_high,
    late_low,
    moved,
    own_sem,
    a_send,
    a_recv,
    x_send,
    x_recv,
    c_send,
    c_recv,
    r_send,
    r_recv,
):
    count, width = rows_ref.shape
    chunk = count // groups
    half = count // 2
    members = shards
    pairs = members // 2
    wide = groups // shards
    near = shards // 2
    b = lax.axis_index("batch")
    s = lax.axis_index("shard")
    q, t = b // members, b % members
    x, c = t // 2, t % 2
    g = q * shards + s
    h, l = s // near, s % near

    def piece(index, start=0, rows=chunk):
        return pl.ds(pl.multiple_of(index * chunk + start, 8), rows)

    def group(step, sign):
        far, i, dq = step
        side = 1 - h if far else h
        column = side * near + lax.rem(l + near + sign * i, near)
        return lax.rem(q + wide + sign * dq, wide) * shards + column

    def place(index):
        return (index // shards) * members + t, index % shards

    def mate(j, other):
        return q * members + lax.rem(x + j, pairs) * 2 + (1 - c if other else c), s

    self_step = (0, 0, 0)
    same = [(0, 0, dq) for dq in range(1, wide)]
    close = [(0, i, dq) for i in range(1, near) for dq in range(wide)]
    far = [(1, i, dq) for i in range(near) for dq in range(wide)]
    mixed_order = []
    for n in range(max(len(far), len(close))):
        mixed_order += far[n : n + 1] + close[n : n + 1]
    steps = [self_step] + same + mixed_order
    items = []
    for n, at in enumerate(steps):
        if n >= groups - 2:
            items += [(at, 0, chunk // 2), (at, chunk // 2, chunk // 2)]
        else:
            items.append((at, 0, chunk))

    barrier = pltpu.get_barrier_semaphore()
    targets = [place(group(at, 1)) for at in steps[1:]]
    targets += [mate(j, False) for j in range(1, pairs)] + [mate(0, True)]
    for target in targets:
        pl.semaphore_signal(barrier, inc=1, device_id=target, device_id_type=MESH)
    pl.semaphore_wait(barrier, len(targets))

    own = pltpu.make_async_copy(rows_ref.at[piece(g)], pool.at[t, piece(g)], own_sem.at[0])
    own.start()
    sends = [own]
    for n, (at, start, rows) in enumerate(items[1:], 1):
        to = group(at, 1)
        sends.append(
            pltpu.make_async_remote_copy(
                src_ref=rows_ref.at[piece(to, start, rows)],
                dst_ref=pool.at[t, piece(g, start, rows)],
                send_sem=a_send.at[n],
                recv_sem=a_recv.at[n],
                device_id=place(to),
                device_id_type=MESH,
            )
        )
        sends[-1].start()

    def pass_on(j, n, other):
        at, start, rows = items[n]
        source = piece(group(at, -1), start, rows)
        block = lax.rem(x + pairs - (j if other else 0), pairs) * 2 + c
        sem = (c_send, c_recv) if other else (x_send, x_recv)
        copy = pltpu.make_async_remote_copy(
            src_ref=pool.at[block, source],
            dst_ref=pool.at[block, source],
            send_sem=sem[0].at[j, n],
            recv_sem=sem[1].at[j, n],
            device_id=mate(0, True) if other else mate(j, False),
            device_id_type=MESH,
        )
        copy.start()
        return copy

    across, inside = {}, {}
    for n in range(len(items)):
        if n == 0:
            own.wait()
        else:
            sends[n].wait_recv()
        for j in range(1, pairs):
            across[j, n] = pass_on(j, n, False)
        inside[0, n] = pass_on(0, n, True)
        if n >= 2:
            for j in range(1, pairs):
                across[j, n - 2].wait_recv()
                inside[j, n - 2] = pass_on(j, n - 2, True)

    means = means_ref[...]
    mean_parts = split(means)
    mean_sq = jnp.sum(means * means, axis=1, keepdims=True)
    back_order = far + close + same + [self_step]
    for n, at in enumerate(back_order):
        block = pool[t, piece(group(at, 1))]
        high, low = split(block)
        spot = slice(n * chunk, (n + 1) * chunk)
        mine[spot, :] = block
        lhs_high[spot, :] = high
        lhs_low[spot, :] = low
        own_sq[spot, :] = jnp.sum(block * block, axis=1, keepdims=True)
    lhs_high[count:, :] = mean_parts[0]
    lhs_low[count:, :] = mean_parts[1]

    def process(block, first):
        points = pool[block]
        parts = split(points)
        sq = jnp.sum(points * points, axis=1, keepdims=True)
        sq_row = jnp.transpose(jnp.broadcast_to(sq, (count, 128)))[0:1, :]
        crossed = dot3((lhs_high[...], lhs_low[...]), parts, ((1,), (1,)))
        kernel = jnp.exp(-(own_sq[...] + sq_row - 2.0 * crossed[:count]) * (2.0 / width))
        logits = logw_ref[...] - (sq_row - 2.0 * crossed[count:] + mean_sq) / (2.0 * variance)
        weights = jnp.exp(logits - jnp.max(logits, axis=0, keepdims=True))
        weights = weights / jnp.sum(weights, axis=0, keepdims=True)
        high, low = split(kernel)
        late_high[block] = high[half:]
        late_low[block] = low[half:]
        point = dot3((high[:half], low[:half]), parts, ((1,), (0,)))
        mixed = dot3((high, low), split(weights), ((1,), (1,)))
        total = jnp.sum(kernel, axis=1, keepdims=True)
        if first:
            acc[...] = point
            acc_w[...] = mixed
            acc_k[...] = total
        else:
            acc[...] += point
            acc_w[...] += mixed
            acc_k[...] += total

    process(t, True)

    for n in range(len(items) - 2, len(items)):
        for j in range(1, pairs):
            across[j, n].wait_recv()
            inside[j, n] = pass_on(j, n, True)
    for copy in inside.values():
        copy.wait_recv()

    def rest(i, carry):
        j, e = i // 2, i % 2
        process(lax.rem(x + pairs - j, pairs) * 2 + lax.rem(c + e, 2), False)
        return carry

    lax.fori_loop(1, members, rest, 0)

    size = count * members
    scale = 4.0 / width
    back = []

    def finish(first):
        span = slice(first, first + half)
        pulled = dot3(split(acc_w[span, :]), mean_parts, ((1,), (0,)))
        rows = mine[span, :]
        drift = (pulled - acc[...]) / variance + scale * (rows * acc_k[span, :] - acc[...])
        moved[span, :] = rows + (step_size / size) * drift
        for n in range(first // chunk, (first + half) // chunk):
            spot = slice(n * chunk, (n + 1) * chunk)
            to = group(back_order[n], 1)
            if n == groups - 1:
                copy = pltpu.make_async_copy(moved.at[spot], out_ref.at[piece(g)], own_sem.at[1])
            else:
                copy = pltpu.make_async_remote_copy(
                    src_ref=moved.at[spot],
                    dst_ref=out_ref.at[piece(g)],
                    send_sem=r_send.at[n],
                    recv_sem=r_recv.at[n],
                    device_id=place(to),
                    device_id_type=MESH,
                )
            copy.start()
            back.append(copy)

    finish(0)

    def later(block, carry):
        point = dot3((late_high[block], late_low[block]), split(pool[block]), ((1,), (0,)))
        acc[...] += point
        return carry

    acc[...] = jnp.zeros_like(acc)
    lax.fori_loop(0, members, later, 0)
    finish(half)

    for copy in sends[1:]:
        copy.wait_send()
    for copy in across.values():
        copy.wait_send()
    for copy in inside.values():
        copy.wait_send()
    for copy in back:
        copy.wait()


def step(rows, means, logw, groups, shards):
    count, width = rows.shape
    components = means.shape[0]
    pairs = shards // 2
    dma = pltpu.SemaphoreType.DMA
    return pl.pallas_call(
        functools.partial(step_kernel, groups, shards),
        out_shape=jax.ShapeDtypeStruct((count, width), jnp.float32),
        in_specs=[pl.BlockSpec(memory_space=pltpu.VMEM)] * 3,
        out_specs=pl.BlockSpec(memory_space=pltpu.VMEM),
        scratch_shapes=[
            pltpu.VMEM((shards, count, width), jnp.float32),
            pltpu.VMEM((count, width), jnp.float32),
            pltpu.VMEM((count + components, width), jnp.bfloat16),
            pltpu.VMEM((count + components, width), jnp.bfloat16),
            pltpu.VMEM((count, 1), jnp.float32),
            pltpu.VMEM((count // 2, width), jnp.float32),
            pltpu.VMEM((count, components), jnp.float32),
            pltpu.VMEM((count, 1), jnp.float32),
            pltpu.VMEM((shards, count // 2, count), jnp.bfloat16),
            pltpu.VMEM((shards, count // 2, count), jnp.bfloat16),
            pltpu.VMEM((count, width), jnp.float32),
            dma((2,)),
            dma((groups + 2,)),
            dma((groups + 2,)),
            dma((pairs, groups + 2)),
            dma((pairs, groups + 2)),
            dma((pairs, groups + 2)),
            dma((pairs, groups + 2)),
            dma((groups,)),
            dma((groups,)),
        ],
        compiler_params=pltpu.CompilerParams(
            collective_id=0, has_side_effects=True, vmem_limit_bytes=48 * 1024 * 1024
        ),
    )(rows, means, logw)


def permutation(batch, groups):
    count = batch.shape[0]
    chunk = count // groups
    index = jnp.arange(count, dtype=jnp.int32)
    same = (batch[:, None] == batch[None, :]) & (index[:, None] < index[None, :])
    spot = batch * chunk + jnp.sum(same.astype(jnp.int32), axis=0)
    return (index[:, None] == spot[None, :]).astype(jnp.float32)


def apply(matrix, rows, transposed=False):
    dims = (((0,), (0,)) if transposed else ((1,), (0,)), ((), ()))
    return lax.dot_general(
        matrix, rows, dims, precision=lax.Precision.HIGHEST, preferred_element_type=jnp.float32
    )


def body(particles, batch_of, mixture_means, log_weights):
    groups = lax.axis_size("batch")
    shards = lax.axis_size("shard")
    logw = log_weights[:, None]
    current = particles
    previous = None
    for iteration in range(batch_of.shape[0]):
        order = permutation(batch_of[iteration], groups)
        if previous is None:
            current = apply(order, current)
        else:
            both = lax.dot_general(
                order.astype(jnp.bfloat16),
                previous.astype(jnp.bfloat16),
                (((1,), (1,)), ((), ())),
                preferred_element_type=jnp.float32,
            )
            current = apply(both, current)
        current = step(current, mixture_means, logw, groups, shards)
        previous = order
    return apply(previous, current, transposed=True)


def solution(mesh):
    placed = (P(("batch", "shard"), None), P(None, ("batch", "shard")), P(), P())
    return jax.shard_map(
        body, mesh=mesh, in_specs=placed, out_specs=P(("batch", "shard"), None), check_vma=False
    )
```

```python
import functools

import jax
import jax.numpy as jnp
from jax import lax
from jax.experimental import pallas as pl
from jax.experimental.pallas import tpu as pltpu
from jax.sharding import PartitionSpec as P

variance = 4.0
step_size = 32.0
MESH = pl.DeviceIdType.MESH


def split(a):
    high = a.astype(jnp.bfloat16)
    return high, (a - high.astype(jnp.float32)).astype(jnp.bfloat16)


def dot3(a, b, contract):
    dims = (contract, ((), ()))
    one = functools.partial(lax.dot_general, dimension_numbers=dims, preferred_element_type=jnp.float32)
    return one(a[0], b[0]) + (one(a[0], b[1]) + one(a[1], b[0]))


def step_kernel(
    groups,
    shards,
    rows_ref,
    means_ref,
    logw_ref,
    out_ref,
    pool,
    mine,
    lhs_high,
    lhs_low,
    own_sq,
    acc,
    acc_w,
    acc_k,
    mix,
    moved,
    own_sem,
    a_send,
    a_recv,
    x_send,
    x_recv,
    c_send,
    c_recv,
    r_send,
    r_recv,
):
    count, width = rows_ref.shape
    chunk = count // groups
    half = count // 2
    components = means_ref.shape[0]
    members = shards
    pairs = members // 2
    wide = groups // shards
    near = shards // 2
    b = lax.axis_index("batch")
    s = lax.axis_index("shard")
    q, t = b // members, b % members
    x, c = t // 2, t % 2
    g = q * shards + s
    h, l = s // near, s % near

    def piece(index, start=0, rows=chunk):
        return pl.ds(pl.multiple_of(index * chunk + start, 8), rows)

    def group(step, sign):
        far, i, dq = step
        side = 1 - h if far else h
        column = side * near + lax.rem(l + near + sign * i, near)
        return lax.rem(q + wide + sign * dq, wide) * shards + column

    def place(index):
        return (index // shards) * members + t, index % shards

    def mate(j, other):
        return q * members + lax.rem(x + j, pairs) * 2 + (1 - c if other else c), s

    self_step = (0, 0, 0)
    same = [(0, 0, dq) for dq in range(1, wide)]
    close = [(0, i, dq) for i in range(1, near) for dq in range(wide)]
    far = [(1, i, dq) for i in range(near) for dq in range(wide)]
    mixed_order = []
    for n in range(max(len(far), len(close))):
        mixed_order += far[n : n + 1] + close[n : n + 1]
    steps = [self_step] + same + mixed_order
    items = []
    for n, at in enumerate(steps):
        if n >= groups - 2:
            items += [(at, 0, chunk // 2), (at, chunk // 2, chunk // 2)]
        else:
            items.append((at, 0, chunk))

    barrier = pltpu.get_barrier_semaphore()
    targets = [place(group(at, 1)) for at in steps[1:]]
    targets += [mate(j, False) for j in range(1, pairs)] + [mate(0, True)]
    for target in targets:
        pl.semaphore_signal(barrier, inc=1, device_id=target, device_id_type=MESH)
    pl.semaphore_wait(barrier, len(targets))

    own = pltpu.make_async_copy(rows_ref.at[piece(g)], pool.at[t, piece(g)], own_sem.at[0])
    own.start()
    sends = [own]
    for n, (at, start, rows) in enumerate(items[1:], 1):
        to = group(at, 1)
        sends.append(
            pltpu.make_async_remote_copy(
                src_ref=rows_ref.at[piece(to, start, rows)],
                dst_ref=pool.at[t, piece(g, start, rows)],
                send_sem=a_send.at[n],
                recv_sem=a_recv.at[n],
                device_id=place(to),
                device_id_type=MESH,
            )
        )
        sends[-1].start()

    def pass_on(j, n, other):
        at, start, rows = items[n]
        source = piece(group(at, -1), start, rows)
        block = lax.rem(x + pairs - (j if other else 0), pairs) * 2 + c
        sem = (c_send, c_recv) if other else (x_send, x_recv)
        copy = pltpu.make_async_remote_copy(
            src_ref=pool.at[block, source],
            dst_ref=pool.at[block, source],
            send_sem=sem[0].at[j, n],
            recv_sem=sem[1].at[j, n],
            device_id=mate(0, True) if other else mate(j, False),
            device_id_type=MESH,
        )
        copy.start()
        return copy

    across, inside = {}, {}
    for n in range(len(items)):
        if n == 0:
            own.wait()
        else:
            sends[n].wait_recv()
        for j in range(1, pairs):
            across[j, n] = pass_on(j, n, False)
        inside[0, n] = pass_on(0, n, True)
        if n >= 2:
            for j in range(1, pairs):
                across[j, n - 2].wait_recv()
                inside[j, n - 2] = pass_on(j, n - 2, True)

    means = means_ref[...]
    mean_parts = split(means)
    mean_sq = jnp.sum(means * means, axis=1, keepdims=True)
    back_order = far + close + same + [self_step]
    for n, at in enumerate(back_order):
        block = pool[t, piece(group(at, 1))]
        high, low = split(block)
        spot = slice(n * chunk, (n + 1) * chunk)
        shift = 0 if n < groups // 2 else components
        left = slice(n * chunk + shift, (n + 1) * chunk + shift)
        mine[spot, :] = block
        lhs_high[left, :] = high
        lhs_low[left, :] = low
        own_sq[spot, :] = jnp.sum(block * block, axis=1, keepdims=True)
    lhs_high[half : half + components, :] = mean_parts[0]
    lhs_low[half : half + components, :] = mean_parts[1]

    def process(block, late, first=False):
        points = pool[block]
        parts = split(points)
        sq = jnp.sum(points * points, axis=1, keepdims=True)
        sq_row = jnp.transpose(jnp.broadcast_to(sq, (count, 128)))[0:1, :]
        span = slice(half, count) if late else slice(0, half)
        left = slice(half + components, None) if late else slice(0, half + components)
        crossed = dot3((lhs_high[left, :], lhs_low[left, :]), parts, ((1,), (1,)))
        kernel = jnp.exp(-(own_sq[span, :] + sq_row - 2.0 * crossed[:half]) * (2.0 / width))
        if late:
            weights = mix[block]
        else:
            logits = logw_ref[...] - (sq_row - 2.0 * crossed[half:] + mean_sq) / (2.0 * variance)
            weights = jnp.exp(logits - jnp.max(logits, axis=0, keepdims=True))
            weights = weights / jnp.sum(weights, axis=0, keepdims=True)
            mix[block] = weights
        kernel_parts = split(kernel)
        point = dot3(kernel_parts, parts, ((1,), (0,)))
        mixed = dot3(kernel_parts, split(weights), ((1,), (1,)))
        total = jnp.sum(kernel, axis=1, keepdims=True)
        if first:
            acc[...] = point
            acc_w[...] = mixed
            acc_k[...] = total
        else:
            acc[...] += point
            acc_w[...] += mixed
            acc_k[...] += total

    process(t, False, True)

    for n in range(len(items) - 2, len(items)):
        for j in range(1, pairs):
            across[j, n].wait_recv()
            inside[j, n] = pass_on(j, n, True)
    for copy in inside.values():
        copy.wait_recv()

    def rest(i, carry):
        j, e = i // 2, i % 2
        process(lax.rem(x + pairs - j, pairs) * 2 + lax.rem(c + e, 2), False)
        return carry

    lax.fori_loop(1, members, rest, 0)

    size = count * members
    scale = 4.0 / width
    back = []

    def finish(first):
        span = slice(first, first + half)
        pulled = dot3(split(acc_w[...]), mean_parts, ((1,), (0,)))
        rows = mine[span, :]
        drift = (pulled - acc[...]) / variance + scale * (rows * acc_k[...] - acc[...])
        moved[span, :] = rows + (step_size / size) * drift
        for n in range(first // chunk, (first + half) // chunk):
            spot = slice(n * chunk, (n + 1) * chunk)
            to = group(back_order[n], 1)
            if n == groups - 1:
                copy = pltpu.make_async_copy(moved.at[spot], out_ref.at[piece(g)], own_sem.at[1])
            else:
                copy = pltpu.make_async_remote_copy(
                    src_ref=moved.at[spot],
                    dst_ref=out_ref.at[piece(g)],
                    send_sem=r_send.at[n],
                    recv_sem=r_recv.at[n],
                    device_id=place(to),
                    device_id_type=MESH,
                )
            copy.start()
            back.append(copy)

    finish(0)

    def later(block, carry):
        process(block, True)
        return carry

    acc[...] = jnp.zeros_like(acc)
    acc_w[...] = jnp.zeros_like(acc_w)
    acc_k[...] = jnp.zeros_like(acc_k)
    lax.fori_loop(0, members, later, 0)
    finish(half)

    for copy in sends[1:]:
        copy.wait_send()
    for copy in across.values():
        copy.wait_send()
    for copy in inside.values():
        copy.wait_send()
    for copy in back:
        copy.wait()


def step(rows, means, logw, groups, shards):
    count, width = rows.shape
    components = means.shape[0]
    pairs = shards // 2
    dma = pltpu.SemaphoreType.DMA
    return pl.pallas_call(
        functools.partial(step_kernel, groups, shards),
        out_shape=jax.ShapeDtypeStruct((count, width), jnp.float32),
        in_specs=[pl.BlockSpec(memory_space=pltpu.VMEM)] * 3,
        out_specs=pl.BlockSpec(memory_space=pltpu.VMEM),
        scratch_shapes=[
            pltpu.VMEM((shards, count, width), jnp.float32),
            pltpu.VMEM((count, width), jnp.float32),
            pltpu.VMEM((count + components, width), jnp.bfloat16),
            pltpu.VMEM((count + components, width), jnp.bfloat16),
            pltpu.VMEM((count, 1), jnp.float32),
            pltpu.VMEM((count // 2, width), jnp.float32),
            pltpu.VMEM((count // 2, components), jnp.float32),
            pltpu.VMEM((count // 2, 1), jnp.float32),
            pltpu.VMEM((shards, components, count), jnp.float32),
            pltpu.VMEM((count, width), jnp.float32),
            dma((2,)),
            dma((groups + 2,)),
            dma((groups + 2,)),
            dma((pairs, groups + 2)),
            dma((pairs, groups + 2)),
            dma((pairs, groups + 2)),
            dma((pairs, groups + 2)),
            dma((groups,)),
            dma((groups,)),
        ],
        compiler_params=pltpu.CompilerParams(
            collective_id=0, has_side_effects=True, vmem_limit_bytes=48 * 1024 * 1024
        ),
    )(rows, means, logw)


def permutation(batch, groups):
    count = batch.shape[0]
    chunk = count // groups
    index = jnp.arange(count, dtype=jnp.int32)
    same = (batch[:, None] == batch[None, :]) & (index[:, None] < index[None, :])
    spot = batch * chunk + jnp.sum(same.astype(jnp.int32), axis=0)
    return (index[:, None] == spot[None, :]).astype(jnp.float32)


def apply(matrix, rows, transposed=False):
    dims = (((0,), (0,)) if transposed else ((1,), (0,)), ((), ()))
    return lax.dot_general(
        matrix, rows, dims, precision=lax.Precision.HIGHEST, preferred_element_type=jnp.float32
    )


def body(particles, batch_of, mixture_means, log_weights):
    groups = lax.axis_size("batch")
    shards = lax.axis_size("shard")
    logw = log_weights[:, None]
    current = particles
    previous = None
    for iteration in range(batch_of.shape[0]):
        order = permutation(batch_of[iteration], groups)
        if previous is None:
            current = apply(order, current)
        else:
            both = lax.dot_general(
                order.astype(jnp.bfloat16),
                previous.astype(jnp.bfloat16),
                (((1,), (1,)), ((), ())),
                preferred_element_type=jnp.float32,
            )
            current = apply(both, current)
        current = step(current, mixture_means, logw, groups, shards)
        previous = order
    return apply(previous, current, transposed=True)


def solution(mesh):
    placed = (P(("batch", "shard"), None), P(None, ("batch", "shard")), P(), P())
    return jax.shard_map(
        body, mesh=mesh, in_specs=placed, out_specs=P(("batch", "shard"), None), check_vma=False
    )
```
